32 devices in a mesh: blk: 16 (over z, y, core), col: 2 (over x).
Axes of the slice: x: 2, y: 2, z: 4, core: 2. Of those that a mesh axis runs over, the one named last changes fastest.
Arguments:
- encodings: bfloat16 [8192, 1024], P(('blk', 'col')), may hold values from -8 to 8
- first_weight: bfloat16 [1024, 512], replicated, may hold values from -0.1875 to 0.1875
- second_weight: bfloat16 [512, 32], replicated, may hold values from -0.25 to 0.25
- inv_scale: float32 [32], replicated, may hold values from 0.2 to 0.8
- outputscale: float32 [1], replicated, may hold values from 0.5 to 2
- noise: float32 [1], replicated, may hold values from 0.2 to 2
- rhs: float32 [32, 8192], P('col', 'blk'), may hold values from -12 to 12
Outputs:
- solution: float32 [32, 8192], P('col', 'blk')
- residual: float32 [32, 8192], P('col', 'blk')
The draws below stay inside these ranges and needn't reach their ends.
All inputs are finite; a program needn't handle non-finite values.
Results may differ from the reference program's by a relative error of at most 0.0079.
Values sent between devices are 32-bit elements; how exact they have to be, the bound alone decides.
A program may use at most 64 MiB of HBM per device.

```python
import math
import jax
import jax.numpy as jnp
from jax import lax

ENC = 1024
HID = 512
FEAT = 32
COLS = 32
ITERS = 1
PTS_DEV = 512
NPTS = 8192


def draw_rhs(key, part):
    position = jnp.arange(NPTS, dtype=jnp.float32) / NPTS
    rising = 1.0 + 2.0 * position
    values = jnp.clip(jax.random.normal(key, (COLS, NPTS), jnp.float32), -4.0, 4.0) * rising[None, :]
    return values


def steps_of(stream_key, dims, cuts, smallest, high):
    def one(dim, shards_of):
        draws = jax.random.uniform(jax.random.fold_in(jax.random.fold_in(stream_key, 6), dim), (shards_of,), jnp.float32, smallest / len(cuts), high / len(cuts))
        return jnp.repeat(jnp.exp(draws), dims[dim] // shards_of).reshape((-1,) + (1,) * (len(dims) - dim - 1))

    loudness = one(*cuts[0])
    for cut in cuts[1:]:
        loudness = loudness * one(*cut)
    return loudness


def bell_draw(stream_key, dims, deviation, bound, pieces=(), kind=jnp.bfloat16):
    array = deviation * jax.random.normal(stream_key, dims, jnp.float32)
    if pieces:
        array = array * steps_of(stream_key, dims, pieces, -0.22, 0.18)
    return jnp.clip(array, -bound, bound).astype(kind)


def setup_inputs(seed: int = 0) -> dict:
    key_of = jax.random.split(jax.random.key(seed), 8)
    encodings = bell_draw(key_of[0], (NPTS, ENC), 2.0, 8.0, ((0, 32),))
    first_weight = bell_draw(key_of[1], (ENC, HID), ENC ** -0.5, 0.1875)
    second_weight = bell_draw(key_of[2], (HID, FEAT), HID ** -0.5, 0.25)
    inv_scale = jnp.clip(jnp.exp(jax.random.uniform(key_of[3], (FEAT,), jnp.float32, math.log(0.2), math.log(0.8))), 0.2, 0.8)
    outputscale = jnp.clip(jax.random.uniform(key_of[4], (1,), jnp.float32, 0.5, 2.0), 0.5, 2.0)
    noise = jnp.clip(jnp.exp(jax.random.uniform(key_of[5], (1,), jnp.float32, math.log(0.2), math.log(2.0))), 0.2, 2.0)
    rhs = draw_rhs(jax.random.fold_in(key_of[7], 71), 0)
    return dict(encodings=encodings, first_weight=first_weight, second_weight=second_weight, inv_scale=inv_scale, outputscale=outputscale, noise=noise, rhs=rhs)


def features_of(encodings, first_weight, second_weight, inv_scale):
    hidden = jnp.maximum(jnp.dot(encodings, first_weight, preferred_element_type=jnp.float32), 0.0).astype(jnp.bfloat16)
    scaled = jnp.dot(hidden, second_weight, preferred_element_type=jnp.float32) * inv_scale[None, :]
    return scaled.T


def apply_kernel(points, vectors, kernel_scale, nugget):
    norms = jnp.sum(points * points, axis=0)
    row_groups = points.reshape(FEAT, NPTS // PTS_DEV, PTS_DEV).transpose(1, 0, 2)

    def one_group(row_points):
        cross = lax.dot_general(row_points, points, (((0,), (0,)), ((), ())), precision=lax.Precision.HIGHEST)
        distance = jnp.sum(row_points * row_points, axis=0)[:, None] + norms[None, :] - 2.0 * cross
        kernel_tile = kernel_scale * jnp.exp(-0.5 * distance)
        return lax.dot_general(vectors, kernel_tile, (((1,), (1,)), ((), ())), precision=lax.Precision.HIGHEST)

    images = lax.map(one_group, row_groups)
    return images.transpose(1, 0, 2).reshape(COLS, NPTS) + nugget * vectors


def reference(encodings, first_weight, second_weight, inv_scale, outputscale, noise, rhs):
    points = features_of(encodings, first_weight, second_weight, inv_scale)
    solution = jnp.zeros_like(rhs)
    residual = rhs
    direction = rhs
    norm_now = jnp.sum(residual * residual, axis=1)
    for sweep in range(ITERS):
        images = apply_kernel(points, direction, outputscale[0], noise[0])
        step_size = norm_now / jnp.sum(direction * images, axis=1)
        solution = solution + step_size[:, None] * direction
        residual = residual - step_size[:, None] * images
        if sweep + 1 < ITERS:
            norm_next = jnp.sum(residual * residual, axis=1)
            direction = residual + (norm_next / norm_now)[:, None] * direction
            norm_now = norm_next
    return solution, residual
```

```python
import functools
import math

import jax
import jax.numpy as jnp
from jax import lax
from jax.experimental import pallas as pl
from jax.experimental.pallas import tpu as pltpu
from jax.sharding import PartitionSpec as P

MESH = pl.DeviceIdType.MESH
F32 = jnp.float32
BF16 = jnp.bfloat16
ROOT_LOG2E = math.sqrt(math.log2(math.e))


def split3(values):
    high = values.astype(BF16)
    rest = values - high.astype(F32)
    mid = rest.astype(BF16)
    low = (rest - mid.astype(F32)).astype(BF16)
    return high, mid, low


def stacked(points, mine):
    width = points.shape[1]
    points = points * ROOT_LOG2E
    high, mid, low = split3(points)
    half_norm = -0.5 * jnp.sum(points * points, axis=0, keepdims=True)
    parts = [part.astype(F32) for part in split3(half_norm)]
    row = lax.broadcasted_iota(jnp.int32, (16, width), 0)
    first = 3 if mine else 0
    extra = jnp.where(row < 6, 1.0, 0.0).astype(F32)
    for at, part in enumerate(parts):
        extra = jnp.where(row == first + at, part, extra)
    extra = extra.astype(BF16)
    order = [high, high, mid, high, low, mid] if mine else [high, mid, high, low, high, mid]
    used = 6 * points.shape[0] + 16
    total = -(-used // 256) * 256
    return jnp.concatenate(order + [extra, jnp.zeros((total - used, width), BF16)], axis=0)


def kernel(
    nblk, ncol,
    enc_hbm, w1_hbm, w2_ref, inv_ref, scale_ref, noise_ref, rhs_hbm,
    sol_ref, res_ref,
    enc, w1, xall, vall, mine_t, acc, bent,
    load_sem, x_recv, v_recv, b_recv,
    x_out_s, x_mid_s, x_col_s, x_core_s, v_out_s, v_mid_s, v_core_s, b_send,
):
    no = nblk // 4
    blk = lax.axis_index("blk")
    col = lax.axis_index("col")
    out, mid, core = blk // 4, (blk // 2) % 2, blk % 2
    width = xall.shape[2]
    steps = ncol * 2 * no

    def blk_of(o, m, c):
        return (o * 2 + m) * 2 + c

    mid_peer = (blk_of(out, 1 - mid, core), col)
    core_peer = (blk_of(out, mid, 1 - core), col)

    barrier = pltpu.get_barrier_semaphore()
    for d in range(1, nblk):
        pl.semaphore_signal(barrier, inc=1, device_id=(lax.rem(blk + d, nblk), col), device_id_type=MESH)
    for d in range(1, ncol):
        pl.semaphore_signal(barrier, inc=1, device_id=(blk, lax.rem(col + d, ncol)), device_id_type=MESH)

    rhs_load = pltpu.make_async_copy(rhs_hbm, vall.at[blk], load_sem.at[0])
    w1_load = pltpu.make_async_copy(w1_hbm, w1, load_sem.at[1])
    enc_load = pltpu.make_async_copy(enc_hbm, enc, load_sem.at[2])
    rhs_load.start()
    enc_load.start()
    w1_load.start()

    def send(ref, at, peer, send_sem, recv_sem):
        return pltpu.make_async_remote_copy(
            src_ref=ref.at[at], dst_ref=ref.at[at], send_sem=send_sem, recv_sem=recv_sem,
            device_id=peer, device_id_type=MESH,
        )

    def x_send(g, peer, sem):
        return send(xall, g, peer, sem, x_recv.at[g])

    def v_send(b, peer, sem):
        return send(vall, b, peer, sem, v_recv.at[b])

    def col_peer(d):
        return (blk, lax.rem(col + d, ncol))

    def out_peer(d):
        return (blk_of(lax.rem(out + d, no), mid, core), col)

    rhs_load.wait()
    pl.semaphore_wait(barrier, nblk - 1 + ncol - 1)
    for d in range(1, no):
        v_send(blk, out_peer(d), v_out_s.at[d]).start()
    v_send(blk, mid_peer, v_mid_s.at[0]).start()
    v_send(blk, core_peer, v_core_s.at[0]).start()

    enc_load.wait()
    w1_load.wait()
    hidden = jnp.maximum(jnp.dot(enc[...], w1[...], preferred_element_type=F32), 0.0).astype(BF16)
    features = jnp.dot(hidden, w2_ref[...], preferred_element_type=F32) * inv_ref[...]
    me = blk * ncol + col
    xall[me] = features.T
    acc[...] = jnp.zeros_like(acc)

    for d in range(1, no):
        x_send(me, out_peer(d), x_out_s.at[d]).start()
    x_send(me, mid_peer, x_mid_s.at[0]).start()
    for d in range(1, ncol):
        x_send(me, col_peer(d), x_col_s.at[d - 1, 0]).start()
    x_send(me, core_peer, x_core_s.at[0]).start()

    for d in range(1, no):
        b = blk_of(lax.rem(out + d, no), mid, core)
        v_send(b, mid_peer, v_mid_s.at[d]).wait_recv()
        v_send(b, mid_peer, v_mid_s.at[d]).start()
        v_send(b, core_peer, v_core_s.at[d]).start()

    for d in range(1, ncol):
        g = blk * ncol + lax.rem(col + d, ncol)
        x_send(g, core_peer, x_core_s.at[0]).wait_recv()
    for k in range(ncol):
        rows = stacked(xall[blk * ncol + k], True)
        mine_t[pl.ds(k * width, width), :] = rows.T

    def place(s):
        dk, dm, do = s // (2 * no), (s // no) % 2, s % no
        o, m, k = lax.rem(out + do, no), lax.rem(mid + dm, 2), lax.rem(col + dk, ncol)
        return dk, dm, do, o, m, k

    def product(b, k):
        rows = stacked(xall[b * ncol + k], False)
        vec = jnp.concatenate(split3(vall[b, :, pl.ds(pl.multiple_of(k * width, width), width)]), axis=0)
        logs = jnp.dot(mine_t[...], rows, preferred_element_type=F32)
        tile = jnp.exp2(logs).astype(BF16)
        return lax.dot_general(tile, vec, (((1,), (1,)), ((), ())), preferred_element_type=F32)

    def step(s, carry):
        dk, dm, do, o, m, k = place(s)
        b = blk_of(o, m, core)
        g = b * ncol + k

        @pl.when(jnp.logical_and(s < steps, s > 0))
        def _():
            @pl.when(jnp.logical_or(dk == 0, s % (2 * no) > 0))
            def _():
                x_send(g, core_peer, x_core_s.at[s]).wait_recv()

            x_send(g, core_peer, x_core_s.at[s]).start()

            @pl.when(dk == 0)
            def _():
                for d in range(1, ncol):
                    x_send(g, col_peer(d), x_col_s.at[d - 1, s]).start()

                @pl.when(dm == 0)
                def _():
                    x_send(g, mid_peer, x_mid_s.at[s]).start()

                @pl.when(dm == 1)
                def _():
                    v_send(b, core_peer, v_core_s.at[s]).wait_recv()
                    v_send(b, core_peer, v_core_s.at[s]).start()

        @pl.when(s >= 2)
        def _():
            dk, dm, do, o, m, k = place(s - 2)
            other = blk_of(o, m, 1 - core)
            x_send(other * ncol + k, core_peer, x_core_s.at[s - 2]).wait_recv()

            @pl.when(dk == 0)
            def _():
                v_send(other, core_peer, v_core_s.at[s - 2]).wait_recv()

            acc[...] += product(blk_of(o, m, core), k) + product(other, k)

        return carry

    lax.fori_loop(0, steps + 2, step, 0)

    rhs = vall[blk]
    count = rhs.shape[0]
    acc_t = acc[...].T
    image = acc_t[:count] + acc_t[count : 2 * count] + acc_t[2 * count :]
    image = scale_ref[0] * image + noise_ref[0] * rhs
    bent[blk] = jnp.broadcast_to(jnp.sum(rhs * image, axis=1, keepdims=True), bent.shape[1:])

    total = jnp.zeros_like(rhs)
    total = lax.fori_loop(0, nblk, lambda b, t: t + vall[b] * vall[b], total)
    norm = jnp.sum(total, axis=1, keepdims=True)

    def bent_send(d, b):
        return send(bent, b, (lax.rem(blk + d, nblk), col), b_send.at[d], b_recv.at[b])

    for d in range(1, nblk):
        bent_send(d, blk).start()
    for d in range(1, nblk):
        bent_send(d, lax.rem(blk + d, nblk)).wait_recv()
    curve = jnp.sum(bent[...], axis=0)[:, :1]
    alpha = norm / curve
    sol_ref[...] = alpha * rhs
    res_ref[...] = rhs - alpha * image

    for d in range(1, nblk):
        bent_send(d, blk).wait_send()
    for d in range(1, no):
        v_send(blk, out_peer(d), v_out_s.at[d]).wait_send()
        x_send(me, out_peer(d), x_out_s.at[d]).wait_send()

    def settle(s, carry):
        x_send(me, core_peer, x_core_s.at[s]).wait_send()

        @pl.when(s < 2 * no)
        def _():
            v_send(blk, core_peer, v_core_s.at[s]).wait_send()
            for d in range(1, ncol):
                x_send(me, core_peer, x_col_s.at[d - 1, s]).wait_send()

        @pl.when(s < no)
        def _():
            x_send(me, core_peer, x_mid_s.at[s]).wait_send()
            v_send(blk, core_peer, v_mid_s.at[s]).wait_send()

        return carry

    lax.fori_loop(0, steps, settle, 0)


def solution(mesh):
    nblk, ncol = mesh.shape["blk"], mesh.shape["col"]
    no = nblk // 4

    def on_device(encodings, first_weight, second_weight, inv_scale, outputscale, noise, rhs):
        half, feat = encodings.shape[0], second_weight.shape[1]
        cols, points = rhs.shape
        depth = -(-(6 * feat + 16) // 256) * 256
        dma = pltpu.SemaphoreType.DMA
        vmem = pl.BlockSpec(memory_space=pltpu.VMEM)
        smem = pl.BlockSpec(memory_space=pltpu.SMEM)
        hbm = pl.BlockSpec(memory_space=pl.ANY)
        out = jax.ShapeDtypeStruct(rhs.shape, F32)
        return pl.pallas_call(
            functools.partial(kernel, nblk, ncol),
            out_shape=(out, out),
            in_specs=[hbm, hbm, vmem, vmem, smem, smem, hbm],
            out_specs=(vmem, vmem),
            scratch_shapes=[
                pltpu.VMEM(encodings.shape, BF16),
                pltpu.VMEM(first_weight.shape, BF16),
                pltpu.VMEM((nblk * ncol, feat, half), F32),
                pltpu.VMEM((nblk, cols, points), F32),
                pltpu.VMEM((points, depth), BF16),
                pltpu.VMEM((points, 3 * cols), F32),
                pltpu.VMEM((nblk, cols, 128), F32),
                dma((3,)),
                dma((nblk * ncol,)),
                dma((nblk,)),
                dma((nblk,)),
                dma((no,)),
                dma((no,)),
                dma((max(ncol - 1, 1), 2 * no)),
                dma((2 * no * ncol,)),
                dma((no,)),
                dma((no,)),
                dma((2 * no,)),
                dma((nblk,)),
            ],
            compiler_params=pltpu.CompilerParams(collective_id=0, has_side_effects=True),
        )(encodings, first_weight, second_weight, inv_scale.reshape(1, feat), outputscale, noise, rhs)

    placed = (P(("blk", "col"), None), P(), P(), P(), P(), P(), P("col", "blk"))
    return jax.shard_map(
        on_device,
        mesh=mesh,
        in_specs=placed,
        out_specs=(P("col", "blk"), P("col", "blk")),
        check_vma=False,
    )
```

```python
import functools
import math

import jax
import jax.numpy as jnp
from jax import lax
from jax.experimental import pallas as pl
from jax.experimental.pallas import tpu as pltpu
from jax.sharding import PartitionSpec as P

MESH = pl.DeviceIdType.MESH
F32 = jnp.float32
BF16 = jnp.bfloat16
ROOT_LOG2E = math.sqrt(math.log2(math.e))


def split3(values):
    high = values.astype(BF16)
    rest = values - high.astype(F32)
    mid = rest.astype(BF16)
    low = (rest - mid.astype(F32)).astype(BF16)
    return high, mid, low


def stacked(points, mine):
    width = points.shape[1]
    points = points * ROOT_LOG2E
    high, mid, low = split3(points)
    half_norm = -0.5 * jnp.sum(points * points, axis=0, keepdims=True)
    parts = [part.astype(F32) for part in split3(half_norm)]
    row = lax.broadcasted_iota(jnp.int32, (16, width), 0)
    first = 3 if mine else 0
    extra = jnp.where(row < 6, 1.0, 0.0).astype(F32)
    for at, part in enumerate(parts):
        extra = jnp.where(row == first + at, part, extra)
    extra = extra.astype(BF16)
    order = [high, high, mid, high, low, mid] if mine else [high, mid, high, low, high, mid]
    used = 6 * points.shape[0] + 16
    total = -(-used // 256) * 256
    return jnp.concatenate(order + [extra, jnp.zeros((total - used, width), BF16)], axis=0)


def to_column(row, count):
    shape = (count, row.shape[1])
    same = lax.broadcasted_iota(jnp.int32, shape, 0) == lax.broadcasted_iota(jnp.int32, shape, 1)
    return jnp.sum(jnp.where(same, row, 0.0), axis=1, keepdims=True)


def to_row(column, width):
    shape = (column.shape[0], width)
    same = lax.broadcasted_iota(jnp.int32, shape, 0) == lax.broadcasted_iota(jnp.int32, shape, 1)
    return jnp.sum(jnp.where(same, column, 0.0), axis=0, keepdims=True)


def kernel(
    nblk, ncol,
    enc_hbm, w1_hbm, w2_hbm, inv_hbm, scale_hbm, noise_hbm, rhs_hbm,
    alpha_ref, image_ref,
    enc, w1, w2_ref, inv_ref, scale_ref, noise_ref, xall, vall, mine_t, acc, bent,
    load_sem, x_recv, v_recv, b_recv,
    x_out_s, x_mid_s, x_col_s, x_core_s, v_out_s, v_mid_s, v_core_s, b_send,
):
    no = nblk // 4
    blk = lax.axis_index("blk")
    col = lax.axis_index("col")
    out, mid, core = blk // 4, (blk // 2) % 2, blk % 2
    width = xall.shape[2]
    steps = ncol * 2 * no

    def blk_of(o, m, c):
        return (o * 2 + m) * 2 + c

    mid_peer = (blk_of(out, 1 - mid, core), col)
    core_peer = (blk_of(out, mid, 1 - core), col)

    barrier = pltpu.get_barrier_semaphore()
    for d in range(1, nblk):
        pl.semaphore_signal(barrier, inc=1, device_id=(lax.rem(blk + d, nblk), col), device_id_type=MESH)
    for d in range(1, ncol):
        pl.semaphore_signal(barrier, inc=1, device_id=(blk, lax.rem(col + d, ncol)), device_id_type=MESH)

    rhs_load = pltpu.make_async_copy(rhs_hbm, vall.at[blk], load_sem.at[0])
    w1_load = pltpu.make_async_copy(w1_hbm, w1, load_sem.at[1])
    enc_load = pltpu.make_async_copy(enc_hbm, enc, load_sem.at[2])
    small_loads = [
        pltpu.make_async_copy(source, target, load_sem.at[3 + at])
        for at, (source, target) in enumerate(
            ((w2_hbm, w2_ref), (inv_hbm, inv_ref), (scale_hbm, scale_ref), (noise_hbm, noise_ref))
        )
    ]
    rhs_load.start()
    enc_load.start()
    w1_load.start()
    for load in small_loads:
        load.start()

    def send(ref, at, peer, send_sem, recv_sem):
        return pltpu.make_async_remote_copy(
            src_ref=ref.at[at], dst_ref=ref.at[at], send_sem=send_sem, recv_sem=recv_sem,
            device_id=peer, device_id_type=MESH,
        )

    def x_send(g, peer, sem):
        return send(xall, g, peer, sem, x_recv.at[g])

    def v_send(b, peer, sem):
        return send(vall, b, peer, sem, v_recv.at[b])

    def col_peer(d):
        return (blk, lax.rem(col + d, ncol))

    def out_peer(d):
        return (blk_of(lax.rem(out + d, no), mid, core), col)

    rhs_load.wait()
    pl.semaphore_wait(barrier, nblk - 1 + ncol - 1)
    for d in range(1, no):
        v_send(blk, out_peer(d), v_out_s.at[d]).start()
    v_send(blk, mid_peer, v_mid_s.at[0]).start()
    v_send(blk, core_peer, v_core_s.at[0]).start()

    for load in small_loads:
        load.wait()
    enc_load.wait()
    w1_load.wait()
    hidden = jnp.maximum(jnp.dot(enc[...], w1[...], preferred_element_type=F32), 0.0).astype(BF16)
    features = lax.dot_general(w2_ref[...], hidden, (((1,), (1,)), ((), ())), preferred_element_type=F32)
    me = blk * ncol + col
    xall[me] = features * to_column(inv_ref[...], features.shape[0])
    acc[...] = jnp.zeros_like(acc)

    for d in range(1, no):
        x_send(me, out_peer(d), x_out_s.at[d]).start()
    x_send(me, mid_peer, x_mid_s.at[0]).start()
    for d in range(1, ncol):
        x_send(me, col_peer(d), x_col_s.at[d - 1, 0]).start()
    x_send(me, core_peer, x_core_s.at[0]).start()

    for d in range(1, no):
        b = blk_of(lax.rem(out + d, no), mid, core)
        v_send(b, mid_peer, v_mid_s.at[d]).wait_recv()
        v_send(b, mid_peer, v_mid_s.at[d]).start()
        v_send(b, core_peer, v_core_s.at[d]).start()

    for d in range(1, ncol):
        g = blk * ncol + lax.rem(col + d, ncol)
        x_send(g, core_peer, x_core_s.at[0]).wait_recv()
    for k in range(ncol):
        rows = stacked(xall[blk * ncol + k], True)
        mine_t[pl.ds(k * width, width), :] = rows.T

    def place(s):
        dk, dm, do = s // (2 * no), (s // no) % 2, s % no
        o, m, k = lax.rem(out + do, no), lax.rem(mid + dm, 2), lax.rem(col + dk, ncol)
        return dk, dm, do, o, m, k

    def product(b, k):
        rows = stacked(xall[b * ncol + k], False)
        vec = jnp.concatenate(split3(vall[b, :, pl.ds(pl.multiple_of(k * width, width), width)]), axis=0)
        logs = jnp.dot(mine_t[...], rows, preferred_element_type=F32)
        tile = jnp.exp2(logs).astype(BF16)
        return lax.dot_general(tile, vec, (((1,), (1,)), ((), ())), preferred_element_type=F32)

    def step(s, carry):
        dk, dm, do, o, m, k = place(s)
        b = blk_of(o, m, core)
        g = b * ncol + k

        @pl.when(jnp.logical_and(s < steps, s > 0))
        def _():
            @pl.when(jnp.logical_or(dk == 0, s % (2 * no) > 0))
            def _():
                x_send(g, core_peer, x_core_s.at[s]).wait_recv()

            x_send(g, core_peer, x_core_s.at[s]).start()

            @pl.when(dk == 0)
            def _():
                for d in range(1, ncol):
                    x_send(g, col_peer(d), x_col_s.at[d - 1, s]).start()

                @pl.when(dm == 0)
                def _():
                    x_send(g, mid_peer, x_mid_s.at[s]).start()

                @pl.when(dm == 1)
                def _():
                    v_send(b, core_peer, v_core_s.at[s]).wait_recv()
                    v_send(b, core_peer, v_core_s.at[s]).start()

        @pl.when(s >= 2)
        def _():
            dk, dm, do, o, m, k = place(s - 2)
            other = blk_of(o, m, 1 - core)
            x_send(other * ncol + k, core_peer, x_core_s.at[s - 2]).wait_recv()

            @pl.when(dk == 0)
            def _():
                v_send(other, core_peer, v_core_s.at[s - 2]).wait_recv()

            acc[...] += product(blk_of(o, m, core), k) + product(other, k)

        return carry

    lax.fori_loop(0, steps + 2, step, 0)

    rhs = vall[blk]
    count = rhs.shape[0]
    acc_t = acc[...].T
    image = acc_t[:count] + acc_t[count : 2 * count] + acc_t[2 * count :]
    image = scale_ref[...] * image + noise_ref[...] * rhs
    image_ref[...] = image
    bent[blk] = to_row(jnp.sum(rhs * image, axis=1, keepdims=True), bent.shape[2])

    total = jnp.zeros_like(rhs)
    total = lax.fori_loop(0, nblk, lambda b, t: t + vall[b] * vall[b], total)
    norm = jnp.sum(total, axis=1, keepdims=True)

    def bent_send(d, b):
        return send(bent, b, (lax.rem(blk + d, nblk), col), b_send.at[d], b_recv.at[b])

    for d in range(1, nblk):
        bent_send(d, blk).start()
    for d in range(1, nblk):
        bent_send(d, lax.rem(blk + d, nblk)).wait_recv()
    curve = to_column(jnp.sum(bent[...], axis=0), count)
    alpha_ref[...] = jnp.broadcast_to(norm / curve, rhs.shape)

    for d in range(1, nblk):
        bent_send(d, blk).wait_send()
    for d in range(1, no):
        v_send(blk, out_peer(d), v_out_s.at[d]).wait_send()
        x_send(me, out_peer(d), x_out_s.at[d]).wait_send()

    def settle(s, carry):
        x_send(me, core_peer, x_core_s.at[s]).wait_send()

        @pl.when(s < 2 * no)
        def _():
            v_send(blk, core_peer, v_core_s.at[s]).wait_send()
            for d in range(1, ncol):
                x_send(me, core_peer, x_col_s.at[d - 1, s]).wait_send()

        @pl.when(s < no)
        def _():
            x_send(me, core_peer, x_mid_s.at[s]).wait_send()
            v_send(blk, core_peer, v_mid_s.at[s]).wait_send()

        return carry

    lax.fori_loop(0, steps, settle, 0)


def solution(mesh):
    nblk, ncol = mesh.shape["blk"], mesh.shape["col"]
    no = nblk // 4

    def on_device(encodings, first_weight, second_weight, inv_scale, outputscale, noise, rhs):
        half, feat = encodings.shape[0], second_weight.shape[1]
        cols, points = rhs.shape
        depth = -(-(6 * feat + 16) // 256) * 256
        dma = pltpu.SemaphoreType.DMA
        vmem = pl.BlockSpec(memory_space=pltpu.VMEM)
        hbm = pl.BlockSpec(memory_space=pl.ANY)
        out = jax.ShapeDtypeStruct(rhs.shape, F32)
        alpha, image = pl.pallas_call(
            functools.partial(kernel, nblk, ncol),
            out_shape=(out, out),
            in_specs=[hbm] * 7,
            out_specs=(vmem, vmem),
            scratch_shapes=[
                pltpu.VMEM(encodings.shape, BF16),
                pltpu.VMEM(first_weight.shape, BF16),
                pltpu.VMEM((feat, second_weight.shape[0]), BF16),
                pltpu.VMEM((1, feat), F32),
                pltpu.VMEM((1, 1), F32),
                pltpu.VMEM((1, 1), F32),
                pltpu.VMEM((nblk * ncol, feat, half), F32),
                pltpu.VMEM((nblk, cols, points), F32),
                pltpu.VMEM((points, depth), BF16),
                pltpu.VMEM((points, 3 * cols), F32),
                pltpu.VMEM((nblk, 1, 128), F32),
                dma((7,)),
                dma((nblk * ncol,)),
                dma((nblk,)),
                dma((nblk,)),
                dma((no,)),
                dma((no,)),
                dma((max(ncol - 1, 1), 2 * no)),
                dma((2 * no * ncol,)),
                dma((no,)),
                dma((no,)),
                dma((2 * no,)),
                dma((nblk,)),
            ],
            compiler_params=pltpu.CompilerParams(collective_id=0, has_side_effects=True),
        )(encodings, first_weight, second_weight.T, inv_scale.reshape(1, feat),
          outputscale.reshape(1, 1), noise.reshape(1, 1), rhs)
        return alpha * rhs, rhs - alpha * image

    placed = (P(("blk", "col"), None), P(), P(), P(), P(), P(), P("col", "blk"))
    return jax.shard_map(
        on_device,
        mesh=mesh,
        in_specs=placed,
        out_specs=(P("col", "blk"), P("col", "blk")),
        check_vma=False,
    )
```

```python
import functools
import math

import jax
import jax.numpy as jnp
from jax import lax
from jax.experimental import pallas as pl
from jax.experimental.pallas import tpu as pltpu
from jax.sharding import PartitionSpec as P

MESH = pl.DeviceIdType.MESH
F32 = jnp.float32
BF16 = jnp.bfloat16
ROOT_LOG2E = math.sqrt(math.log2(math.e))


def split3(values):
    high = values.astype(BF16)
    rest = values - high.astype(F32)
    mid = rest.astype(BF16)
    low = (rest - mid.astype(F32)).astype(BF16)
    return high, mid, low


def stacked(points, mine):
    width = points.shape[1]
    points = points * ROOT_LOG2E
    high, mid, low = split3(points)
    half_norm = -0.5 * jnp.sum(points * points, axis=0, keepdims=True)
    parts = [part.astype(F32) for part in split3(half_norm)]
    row = lax.broadcasted_iota(jnp.int32, (16, width), 0)
    first = 3 if mine else 0
    extra = jnp.where(row < 6, 1.0, 0.0).astype(F32)
    for at, part in enumerate(parts):
        extra = jnp.where(row == first + at, part, extra)
    extra = extra.astype(BF16)
    order = [high, high, mid, high, low, mid] if mine else [high, mid, high, low, high, mid]
    used = 6 * points.shape[0] + 16
    total = -(-used // 256) * 256
    return jnp.concatenate(order + [extra, jnp.zeros((total - used, width), BF16)], axis=0)


def to_column(row, count, first):
    shape = (count, row.shape[1])
    same = lax.broadcasted_iota(jnp.int32, shape, 0) + first == lax.broadcasted_iota(jnp.int32, shape, 1)
    return jnp.sum(jnp.where(same, row, 0.0), axis=1, keepdims=True)


def to_row(column, width):
    shape = (column.shape[0], width)
    same = lax.broadcasted_iota(jnp.int32, shape, 0) == lax.broadcasted_iota(jnp.int32, shape, 1)
    return jnp.sum(jnp.where(same, column, 0.0), axis=0, keepdims=True)


def kernel(
    nblk, ncol,
    enc_hbm, w1_hbm, w2_hbm, inv_hbm, rhs_hbm,
    norm_ref, curve_ref, image_ref,
    enc, w1, w2_ref, inv_ref, xall, vall, rall, mine_t, acc, images, parts, sums,
    load_sem, x_recv, v_recv, r_recv, i_recv, s_recv,
    x_out_s, x_mid_s, x_col_s, x_core_s, v_out_s, v_mid_s, v_core_s, r_send, i_send, s_send,
):
    no = nblk // 4
    everyone = nblk * ncol
    blk = lax.axis_index("blk")
    col = lax.axis_index("col")
    out, mid, core = blk // 4, (blk // 2) % 2, blk % 2
    me = blk * ncol + col
    width = xall.shape[2]
    count = rall.shape[1]
    steps = 2 * no

    def blk_of(o, m, c):
        return (o * 2 + m) * 2 + c

    mid_peer = (blk_of(out, 1 - mid, core), col)
    core_peer = (blk_of(out, mid, 1 - core), col)

    def col_of(d):
        return lax.rem(col + d, ncol)

    def out_of(d):
        return blk_of(lax.rem(out + d, no), mid, core)

    def any_of(d):
        other = lax.rem(me + d, everyone)
        return other, (other // ncol, lax.rem(other, ncol))

    barrier = pltpu.get_barrier_semaphore()
    for d in range(1, everyone):
        pl.semaphore_signal(barrier, inc=1, device_id=any_of(d)[1], device_id_type=MESH)

    def half(k):
        return pl.ds(pl.multiple_of(k * width, width), width)

    my_rows = pl.ds(pl.multiple_of(col * count, count), count)
    loads = [
        pltpu.make_async_copy(source, target, load_sem.at[at])
        for at, (source, target) in enumerate(
            (
                (rhs_hbm, rall.at[col]),
                (rhs_hbm.at[:, half(col)], vall.at[blk, my_rows]),
                (enc_hbm, enc),
                (w1_hbm, w1),
                (w2_hbm, w2_ref),
                (inv_hbm, inv_ref),
            )
        )
    ]
    for load in loads:
        load.start()

    def remote(source, target, peer, send_sem, recv_sem):
        return pltpu.make_async_remote_copy(
            src_ref=source, dst_ref=target, send_sem=send_sem, recv_sem=recv_sem,
            device_id=peer, device_id_type=MESH,
        )

    def x_send(b, peer, sem):
        return remote(xall.at[b], xall.at[b], peer, sem, x_recv.at[b])

    def x_col_send(d):
        return remote(xall.at[blk], xall.at[nblk + col], (blk, col_of(d)), x_col_s.at[d], x_recv.at[nblk + col])

    def v_send(b, peer, sem):
        return remote(vall.at[b], vall.at[b], peer, sem, v_recv.at[b])

    def v_part(do, dk):
        k = col_of(dk)
        return remote(
            rall.at[col, :, half(k)], vall.at[blk, my_rows], (out_of(do), k), v_out_s.at[do, dk], v_recv.at[blk]
        )

    def r_copy(d):
        return remote(rall.at[col], rall.at[col], (blk, col_of(d)), r_send.at[d], r_recv.at[col])

    pieces = [(do, dk) for do in range(no) for dk in range(ncol) if do or dk]
    loads[0].wait()
    loads[1].wait()
    pl.semaphore_wait(barrier, everyone - 1)
    for do, dk in pieces:
        v_part(do, dk).start()

    for load in loads[2:]:
        load.wait()
    hidden = jnp.maximum(jnp.dot(enc[...], w1[...], preferred_element_type=F32), 0.0).astype(BF16)
    features = lax.dot_general(w2_ref[...], hidden, (((1,), (1,)), ((), ())), preferred_element_type=F32)
    xall[blk] = features * to_column(inv_ref[...], features.shape[0], 0)
    acc[...] = jnp.zeros_like(acc)

    for d in range(1, no):
        x_send(blk, (out_of(d), col), x_out_s.at[d]).start()
    x_send(blk, mid_peer, x_mid_s.at[0]).start()
    for d in range(1, ncol):
        x_col_send(d).start()
    x_send(blk, core_peer, x_core_s.at[0]).start()
    for d in range(1, ncol):
        r_copy(d).start()

    for dk in range(1, ncol):
        remote(
            vall.at[blk, my_rows], vall.at[blk, my_rows], core_peer, v_core_s.at[0], v_recv.at[blk]
        ).wait_recv()
    v_send(blk, mid_peer, v_mid_s.at[0]).start()
    v_send(blk, core_peer, v_core_s.at[0]).start()
    for d in range(1, no):
        b = out_of(d)
        v_send(b, mid_peer, v_mid_s.at[d]).wait_recv()
        v_send(b, mid_peer, v_mid_s.at[d]).start()
        v_send(b, core_peer, v_core_s.at[d]).start()

    mine_t[half(col), :] = stacked(xall[blk], True).T
    for d in range(1, ncol):
        k = col_of(d)
        x_send(nblk + k, core_peer, x_core_s.at[0]).wait_recv()
        mine_t[half(k), :] = stacked(xall[nblk + k], True).T

    def place(s):
        dm, do = s // no, s % no
        return lax.rem(out + do, no), lax.rem(mid + dm, 2)

    def product(b):
        rows = stacked(xall[b], False)
        vec = jnp.concatenate(split3(vall[b]), axis=0)
        logs = jnp.dot(mine_t[...], rows, preferred_element_type=F32)
        tile = jnp.exp2(logs).astype(BF16)
        return lax.dot_general(tile, vec, (((1,), (1,)), ((), ())), preferred_element_type=F32)

    def step(s, carry):
        @pl.when(jnp.logical_and(s < steps, s > 0))
        def _():
            o, m = place(s)
            b = blk_of(o, m, core)
            x_send(b, core_peer, x_core_s.at[s]).wait_recv()

            @pl.when(s < no)
            def _():
                x_send(b, mid_peer, x_mid_s.at[s]).start()

            x_send(b, core_peer, x_core_s.at[s]).start()

            @pl.when(s >= no)
            def _():
                v_send(b, core_peer, v_core_s.at[s]).wait_recv()
                v_send(b, core_peer, v_core_s.at[s]).start()

        @pl.when(s >= 2)
        def _():
            o, m = place(s - 2)
            other = blk_of(o, m, 1 - core)
            x_send(other, core_peer, x_core_s.at[s - 2]).wait_recv()
            v_send(other, core_peer, v_core_s.at[s - 2]).wait_recv()
            acc[...] += product(blk_of(o, m, core)) + product(other)

        return carry

    lax.fori_loop(0, steps + 2, step, 0)

    total = count * ncol
    acc_t = acc[...].T
    image = acc_t[:total] + acc_t[total : 2 * total] + acc_t[2 * total :]
    for k in range(ncol):
        images[k] = image[k * count : (k + 1) * count]

    def i_copy(d):
        return remote(images.at[col_of(d)], parts.at[col], (blk, col_of(d)), i_send.at[d], i_recv.at[col])

    def s_copy(d, at):
        return remote(sums.at[at], sums.at[at], any_of(d)[1], s_send.at[d], s_recv.at[at])

    for d in range(1, ncol):
        k = col_of(d)
        remote(rall.at[k], rall.at[k], (blk, k), r_send.at[d], r_recv.at[k]).wait_recv()
    bent = jnp.concatenate(
        [jnp.sum(rall[k] * image[k * count : (k + 1) * count], axis=1, keepdims=True) for k in range(ncol)], axis=0
    )
    norm = jnp.sum(vall[blk] * vall[blk], axis=1, keepdims=True)
    sums[me] = jnp.concatenate([to_row(bent, sums.shape[2]), to_row(norm, sums.shape[2])], axis=0)
    for d in range(1, everyone):
        s_copy(d, me).start()
    for d in range(1, ncol):
        i_copy(d).start()

    final = images[col]
    for d in range(1, ncol):
        k = col_of(d)
        remote(images.at[k], parts.at[k], (blk, k), i_send.at[d], i_recv.at[k]).wait_recv()
        final = final + parts[k]
    image_ref[...] = final
    for d in range(1, everyone):
        s_copy(d, any_of(d)[0]).wait_recv()
    whole = jnp.sum(sums[...], axis=0)
    curve_ref[...] = jnp.broadcast_to(to_column(whole[:1], count, col * count), final.shape)
    norm_ref[...] = jnp.broadcast_to(to_column(whole[1:], count, col * count), final.shape)

    for d in range(1, everyone):
        s_copy(d, me).wait_send()
    for d in range(1, ncol):
        i_copy(d).wait_send()
        r_copy(d).wait_send()
        x_col_send(d).wait_send()
    for do, dk in pieces:
        v_part(do, dk).wait_send()
    for d in range(1, no):
        x_send(blk, (out_of(d), col), x_out_s.at[d]).wait_send()

    def settle(s, carry):
        x_send(blk, core_peer, x_core_s.at[s]).wait_send()
        v_send(blk, core_peer, v_core_s.at[s]).wait_send()

        @pl.when(s < no)
        def _():
            x_send(blk, mid_peer, x_mid_s.at[s]).wait_send()
            v_send(blk, mid_peer, v_mid_s.at[s]).wait_send()

        return carry

    lax.fori_loop(0, steps, settle, 0)


def solution(mesh):
    nblk, ncol = mesh.shape["blk"], mesh.shape["col"]
    no = nblk // 4

    def on_device(encodings, first_weight, second_weight, inv_scale, outputscale, noise, rhs):
        half, feat = encodings.shape[0], second_weight.shape[1]
        cols, points = rhs.shape
        depth = -(-(6 * feat + 16) // 256) * 256
        dma = pltpu.SemaphoreType.DMA
        vmem = pl.BlockSpec(memory_space=pltpu.VMEM)
        hbm = pl.BlockSpec(memory_space=pl.ANY)
        out = jax.ShapeDtypeStruct(rhs.shape, F32)
        norm, curve, image = pl.pallas_call(
            functools.partial(kernel, nblk, ncol),
            out_shape=(out, out, out),
            in_specs=[hbm] * 5,
            out_specs=(vmem, vmem, vmem),
            scratch_shapes=[
                pltpu.VMEM(encodings.shape, BF16),
                pltpu.VMEM(first_weight.shape, BF16),
                pltpu.VMEM((feat, second_weight.shape[0]), BF16),
                pltpu.VMEM((1, feat), F32),
                pltpu.VMEM((nblk + ncol, feat, half), F32),
                pltpu.VMEM((nblk, ncol * cols, half), F32),
                pltpu.VMEM((ncol, cols, points), F32),
                pltpu.VMEM((points, depth), BF16),
                pltpu.VMEM((points, 3 * ncol * cols), F32),
                pltpu.VMEM((ncol, cols, points), F32),
                pltpu.VMEM((ncol, cols, points), F32),
                pltpu.VMEM((nblk * ncol, 2, 128), F32),
                dma((6,)),
                dma((nblk + ncol,)),
                dma((nblk,)),
                dma((ncol,)),
                dma((ncol,)),
                dma((nblk * ncol,)),
                dma((no,)),
                dma((no,)),
                dma((ncol,)),
                dma((2 * no,)),
                dma((no, ncol)),
                dma((no,)),
                dma((2 * no,)),
                dma((ncol,)),
                dma((ncol,)),
                dma((nblk * ncol,)),
            ],
            compiler_params=pltpu.CompilerParams(collective_id=0, has_side_effects=True),
        )(encodings, first_weight, second_weight.T, inv_scale.reshape(1, feat), rhs)
        alpha = norm / (outputscale * curve + noise * norm)
        return alpha * rhs, rhs - alpha * (outputscale * image + noise * rhs)

    placed = (P(("blk", "col"), None), P(), P(), P(), P(), P(), P("col", "blk"))
    return jax.shard_map(
        on_device,
        mesh=mesh,
        in_specs=placed,
        out_specs=(P("col", "blk"), P("col", "blk")),
        check_vma=False,
    )
```
